32 devices in a mesh: band: 2 (over x), tm: 16 (over z, y, core).
Axes of the slice: x: 2, y: 2, z: 4, core: 2. Of those that a mesh axis runs over, the one named last changes fastest.
Arguments:
- voltages: bfloat16 [16, 2, 512, 4096], P('band', None, None, 'tm'), parts along dimension 0, may hold values from -12 to 12
- antenna_flags: int32 [32, 16], P('tm', 'band'), parts along dimension 1, may hold values from -2147483648 to 2147483647, as said below
- owned_tile: int32 [16], replicated, may hold values from 0 to 15, each once
Outputs:
- visibility: float32 [512, 16, 2, 512], P('tm', 'band'), parts along dimension 1
The draws below stay inside these ranges and needn't reach their ends.
There are 2 independent parts, one for each index of `band`. The reference program is written for one: setup_inputs(seed, part) draws one part's arguments, and reference() takes and returns one part's arrays. A program takes and returns all parts, laid end to end along the dimension named above; an argument that names none is the same for every part. Nothing has to cross between parts.
Inputs may be any that keep to these rules, and one draw needn't show every extreme that they name: `antenna_flags`: bit b of word w of sub-integration s is 1 where the samples of both polarisations of antenna 32 * w + b are good in that sub-integration of 128 samples, 0 where flagged; all 32 bits of a word are used; some antennas may be flagged in every sub-integration. A permutation: the index k of tm holds the baseline rows of tile owned_tile[k].
All inputs are finite; a program needn't handle non-finite values.
Results may differ from the reference program's by a relative error of at most 0.0003.
Values sent between devices are 32-bit elements; how exact they have to be, the bound alone decides.
No kernel may reach another device: no remote copies, remote signals or barrier semaphores. Data moves between devices by JAX's collectives and lax.ppermute only.
A program may use at most 128 MiB of HBM per device.

```python
import math
import jax
import jax.numpy as jnp
from jax import lax

ANTENNAS = 256
INPUTS = 512
FLAG_WORDS = 8
CHANS = 8
SAMPLES_DEV = 256
SUB_LEN = 128
SUBS = 32
TIME = 4096
TILES = 16
N_TM = 16


def gains(key, lowest, highest):
    key_amplitude, key_phase = jax.random.split(key)
    amplitude = jnp.exp(jax.random.uniform(key_amplitude, (INPUTS,), jnp.float32, math.log(lowest), math.log(highest)))
    phase = jax.random.uniform(key_phase, (INPUTS,), jnp.float32, -math.pi, math.pi)
    return (amplitude * jnp.cos(phase), amplitude * jnp.sin(phase))


def source_term(key, lowest, highest):
    key_sky, key_gain = jax.random.split(key)
    sky = jax.random.normal(key_sky, (CHANS, 2, 1, TIME), jnp.float32)
    gain_real, gain_imag = gains(key_gain, lowest, highest)
    gain_real = gain_real[None, :, None]
    gain_imag = gain_imag[None, :, None]
    real_term = gain_real * sky[:, 0] - gain_imag * sky[:, 1]
    imag_term = gain_real * sky[:, 1] + gain_imag * sky[:, 0]
    return jnp.stack([real_term, imag_term], axis=1)


def draw_voltages(key, part):
    key_first = jax.random.fold_in(jax.random.fold_in(key, 11), 0)
    key_noise = jax.random.fold_in(jax.random.fold_in(key, 11), 2)
    noise = jax.random.normal(key_noise, (CHANS, 2, INPUTS, TIME), jnp.float32)
    signal = source_term(key_first, 0.5, 2.0)
    return jnp.clip(signal + noise, -12.0, 12.0).astype(jnp.bfloat16)


def draw_antenna_flags(key, part):
    key_rolled, key_dead = jax.random.split(jax.random.fold_in(key, 23))
    sub_position = jnp.arange(SUBS, dtype=jnp.int32)[:, None]
    threshold = 30 + 60 * sub_position // max(SUBS - 1, 1)
    rolled = jax.random.randint(key_rolled, (SUBS, ANTENNAS), 0, 100)
    ranking = jax.random.permutation(key_dead, ANTENNAS)
    alive = ranking >= max(1, ANTENNAS // 64)
    bits = jnp.where(alive[None, :] & (rolled < threshold), 1, 0).astype(jnp.int32)
    bits = bits.reshape(SUBS, FLAG_WORDS, 32)
    shifts = jnp.arange(32, dtype=jnp.int32)
    return jnp.sum(jnp.left_shift(bits, shifts[None, None, :]), axis=-1, dtype=jnp.int32)


def setup_inputs(seed: int = 0, part: int = 0) -> dict:
    key_list = jax.random.split(jax.random.key(seed), 4)
    own_keys = jax.random.split(jax.random.fold_in(key_list[3], part), 4)
    voltages = draw_voltages(jax.random.fold_in(jax.random.fold_in(key_list[3], part), 71), part)
    antenna_flags = draw_antenna_flags(jax.random.fold_in(jax.random.fold_in(key_list[3], part), 71), part)
    owned_tile = jax.random.permutation(key_list[2], TILES).astype(jnp.int32)
    return {"voltages": voltages, "antenna_flags": antenna_flags, "owned_tile": owned_tile}


def unpack_flags(words):
    shifts = jnp.arange(32, dtype=jnp.int32)
    bits = jnp.bitwise_and(jnp.right_shift(words[:, :, None], shifts[None, None, :]), 1)
    return bits.reshape(words.shape[0], words.shape[1] * 32).astype(jnp.int32)


def reference(voltages, antenna_flags, owned_tile):
    channels = voltages.shape[0]
    inputs = voltages.shape[2]
    block_rows = inputs // N_TM
    good = unpack_flags(antenna_flags)
    input_flags = jnp.repeat(good, 2, axis=1)
    sample_flags = jnp.repeat(input_flags.T, SUB_LEN, axis=1).astype(jnp.bfloat16)
    masked = voltages * sample_flags[None, None]

    def add_block(running, block_index):
        segment = lax.dynamic_slice_in_dim(masked, block_index * SAMPLES_DEV, SAMPLES_DEV, 3).astype(jnp.float32)
        real_part = segment[:, 0]
        imag_part = segment[:, 1]
        right_side = jnp.concatenate([real_part, imag_part], axis=-1)
        left_side = jnp.stack([right_side, jnp.concatenate([imag_part, -real_part], axis=-1)], axis=1)
        return running + jnp.einsum("ckiu,cju->ckij", left_side, right_side), None

    initial = jnp.zeros((channels, 2, inputs, inputs), jnp.float32)
    gram = lax.scan(add_block, initial, jnp.arange(N_TM, dtype=jnp.int32))[0]
    counts = SUB_LEN * jnp.dot(good.T, good)
    row_index = (owned_tile[:, None] * block_rows + jnp.arange(block_rows, dtype=jnp.int32)[None, :]).reshape(-1)
    pair_counts = jnp.repeat(jnp.repeat(counts, 2, axis=0), 2, axis=1)[row_index]
    ordered = jnp.transpose(gram[:, :, row_index, :], (2, 0, 1, 3))
    return ordered / jnp.maximum(pair_counts, 1).astype(jnp.float32)[:, None, None, :]
```

```python
import jax
import jax.numpy as jnp
from jax import lax
from jax.experimental import pallas as pl
from jax.experimental.pallas import tpu as pltpu
from jax.sharding import PartitionSpec as P


LANES = 128


def unpack_flags(words):
    shifts = jnp.arange(32, dtype=jnp.int32)
    bits = jnp.bitwise_and(jnp.right_shift(words[:, :, None], shifts[None, None, :]), 1)
    return bits.reshape(words.shape[0], words.shape[1] * 32)


def stack_operands(masked):
    real_part = masked[:, 0]
    imag_part = masked[:, 1]
    right_side = jnp.concatenate([real_part, imag_part], axis=-1)
    left_side = jnp.stack([right_side, jnp.concatenate([imag_part, -real_part], axis=-1)], axis=1)
    return (left_side, right_side)


def plain_shards(voltages, antenna_flags, owned_tile):
    axis_count = lax.axis_size("tm")
    my_index = lax.axis_index("tm")
    inputs = voltages.shape[2]
    samples = voltages.shape[3]
    block_rows = inputs // axis_count
    sub_length = samples // antenna_flags.shape[0]
    every_word = lax.all_gather(antenna_flags, "tm", axis=0, tiled=True)
    every_flag = unpack_flags(every_word)
    local_flag = unpack_flags(antenna_flags)
    own_tile = owned_tile[my_index]
    own_antennas = (own_tile * block_rows + jnp.arange(block_rows, dtype=jnp.int32)) // 2
    own_flags = jnp.take(every_flag, own_antennas, axis=1)
    input_flags = jnp.repeat(every_flag, 2, axis=1)
    counts = sub_length * jnp.dot(own_flags.T, input_flags)
    divisor = jnp.maximum(counts, 1).astype(jnp.float32)[:, None, None, :]
    sample_flags = jnp.repeat(jnp.repeat(local_flag, 2, axis=1).T, sub_length, axis=1).astype(
        jnp.bfloat16
    )
    masked = voltages * sample_flags[None, None]
    left_side, right_side = stack_operands(masked)
    row_index = (
        owned_tile[:, None] * block_rows + jnp.arange(block_rows, dtype=jnp.int32)[None, :]
    ).reshape(-1)
    picked = jnp.take(left_side, row_index, axis=2)
    summed = lax.psum_scatter(
        jnp.einsum("ckru,cju->rckj", picked, right_side, preferred_element_type=jnp.float32),
        "tm",
        scatter_dimension=0,
        tiled=True,
    )
    return summed / divisor


def line_of_chips(mesh):
    columns = mesh.devices.reshape(-1, mesh.shape["tm"])
    count = columns.shape[1]
    if count % 4:
        return None
    for column in columns:
        places = []
        for device in column:
            coords = getattr(device, "coords", None)
            core = getattr(device, "core_on_chip", None)
            if coords is None or core is None:
                return None
            places.append((coords[2], coords[1], coords[0], core))
        zs = sorted({p[0] for p in places})
        ys = sorted({p[1] for p in places})
        if len(ys) != 2 or len({p[2] for p in places}) != 1 or len(zs) * 4 != count:
            return None
        want = [(z, y, places[0][2], core) for z in zs for y in ys for core in (0, 1)]
        if places != want:
            return None
    return count // 4


def fill_mask(mask_ref, tile_ref, flag_ref, slots, rows, subs, sub_length):
    antennas = rows // 2
    row = lax.broadcasted_iota(jnp.int32, (rows, sub_length), 0)
    for k in range(slots):
        first = tile_ref[k] * antennas
        shift = first % 32 + row // 2
        for s in range(subs):
            word = flag_ref[s, first // 32]
            bit = lax.shift_right_arithmetic(jnp.full((rows, sub_length), word, jnp.int32), shift) & 1
            mask_ref[k * rows : (k + 1) * rows, s * sub_length : (s + 1) * sub_length] = bit.astype(
                jnp.float32
            ).astype(jnp.bfloat16)


def gram_step(c, x_ref, T, y, core, own_ref, send_ref, p_ref, *, groups, rows, half):
    quarter = LANES // rows
    span = groups // 2 + 1

    def both(g):
        at = pl.ds(pl.multiple_of(g * LANES, LANES), LANES)
        return x_ref[0, 0, at, :], x_ref[0, 1, at, :]

    real, imag = both(T)
    left = jnp.concatenate(
        [jnp.concatenate([real, imag], axis=1), jnp.concatenate([imag, -real], axis=1)], axis=0
    )
    right = jnp.concatenate(
        [jnp.concatenate(both((T + g) % groups), axis=1) for g in range(span)], axis=0
    )
    p_ref[...] = lax.dot_general(
        left, right, (((1,), (1,)), ((), ())), preferred_element_type=jnp.float32
    )
    lane = lax.broadcasted_iota(jnp.int32, (rows, LANES), 1)
    edge = slice((span - 1) * LANES, span * LANES)
    mine = (c < half) == (T < groups // 2)
    j = c % half
    main = 2 * half * 2 * (span - 1)
    for dest, parity in ((own_ref, core), (send_ref, 1 - core)):
        for slot_y in range(2):
            r = 2 * (y if slot_y == 0 else 1 - y) + parity
            shift = r * rows
            for ri in range(2):
                at = pl.ds(pl.multiple_of(ri * LANES + shift, rows), rows)
                last = p_ref[at, edge]
                for g in range(span - 1):
                    block = p_ref[at, g * LANES : (g + 1) * LANES]
                    if g == 0:
                        block = jnp.where(lane < shift, last, block)
                    dest[slot_y, (c * 2 + ri) * (span - 1) + g] = block

                @pl.when(mine)
                def _():
                    moved = pltpu.roll(last, (rows * (j - r + quarter)) % LANES, axis=1)
                    old = dest[slot_y, main + ri]
                    dest[slot_y, main + ri] = jnp.where(lane // rows == j, moved, old)


def first_kernel(
    place_ref, tile_ref, flag_ref, v_ref, x_ref, own_ref, send_ref, mask_ref, p_ref, *, slots, rows, subs, **kw
):
    c = pl.program_id(0)

    @pl.when(c == 0)
    def _():
        fill_mask(mask_ref, tile_ref, flag_ref, slots, rows, subs, v_ref.shape[3] // subs)

    for k in range(slots):
        at = pl.ds(pl.multiple_of(tile_ref[k] * rows, rows), rows)
        for ri in range(2):
            x_ref[0, ri, k * rows : (k + 1) * rows, :] = (
                v_ref[0, ri, at, :] * mask_ref[k * rows : (k + 1) * rows, :]
            )
    gram_step(c, x_ref, place_ref[0], place_ref[1], place_ref[2], own_ref, send_ref, p_ref, rows=rows, **kw)


def next_kernel(place_ref, x_ref, own_ref, send_ref, p_ref, **kw):
    gram_step(
        pl.program_id(0), x_ref, place_ref[0], place_ref[1], place_ref[2], own_ref, send_ref, p_ref, **kw
    )


def mirror_kernel(place_ref, a_ref, b_ref, c_ref, d_ref, z_ref, *refs, channels, rows, slots, span):
    messages, tr_ref = refs[:-1], refs[-1]
    r = place_ref[1] * 2 + place_ref[2]
    quarter = LANES // rows
    cells = (span - 1) * quarter
    z_ref[...] = (a_ref[...] + b_ref[...]) + (c_ref[...] + d_ref[...])
    packs = channels // quarter
    for ri in range(2):
        for g in range(span - 1):
            for h in range(packs):
                block = jnp.concatenate(
                    [z_ref[((h * quarter + j) * 2 + ri) * (span - 1) + g] for j in range(quarter)], axis=0
                )
                turned = block.T
                tr_ref[g, ri * packs + h] = -turned if ri else turned
    for delta in range(1, cells):
        q = (r + delta) % cells
        at = pl.ds(pl.multiple_of((q % quarter) * rows, rows), rows)
        for i in range(2 * packs):
            messages[delta - 1][i] = tr_ref[q // quarter, i, at, :]
    lane = lax.broadcasted_iota(jnp.int32, (rows, LANES), 1)
    main = channels * 2 * (span - 1)
    for ri in range(2):
        turned = jnp.concatenate([z_ref[main + ri]] * quarter, axis=0).T
        piece = turned[0:rows]
        for j in range(1, quarter):
            piece = jnp.where(lane // rows == j, turned[j * rows : (j + 1) * rows], piece)
        messages[cells - 1][ri] = -piece if ri else piece


def scale_kernel(place_ref, tile_ref, word_ref, out_ref, count_ref, *, rows, sub_length):
    inputs = out_ref.shape[1]
    words = word_ref[...]
    subs = words.shape[0]
    lane = lax.broadcasted_iota(jnp.int32, (subs, LANES), 1)
    parts = []
    for g in range(inputs // LANES):
        low, high = words[:, 2 * g : 2 * g + 1], words[:, 2 * g + 1 : 2 * g + 2]
        word = jnp.where(lane < LANES // 2, low, high)
        parts.append(lax.shift_right_arithmetic(word, (lane % (LANES // 2)) // 2) & 1)
    good = jnp.concatenate(parts, axis=1).astype(jnp.float32)
    count_ref[...] = lax.dot_general(
        good, good, (((0,), (0,)), ((), ())), preferred_element_type=jnp.float32
    )
    first = pl.multiple_of(tile_ref[place_ref[3]] * rows, rows)
    counts = count_ref[pl.ds(first, rows), :] * float(sub_length)
    out_ref[...] = 1.0 / jnp.maximum(counts, 1.0)


def final_kernel(place_ref, tile_ref, z_ref, scale_ref, *refs, channels, rows, slots, span):
    messages, out_ref, acc_ref = refs[:-2], refs[-2], refs[-1]
    me = place_ref[3]
    r = place_ref[1] * 2 + place_ref[2]
    quarter = LANES // rows
    cells = (span - 1) * quarter
    packs = channels // quarter
    half = channels // 2
    main = channels * 2 * (span - 1)
    lane = lax.broadcasted_iota(jnp.int32, (rows, LANES), 1) // rows
    low = me < slots // 2

    def body(c, carry):
        j = c % quarter
        h = c // quarter
        for delta in range(slots):
            tile = tile_ref[(me + delta) % slots]
            there = tile % quarter
            group = tile // quarter
            for ri in range(2):
                if delta < cells:
                    q = (r + delta) % cells
                    source = z_ref[(c * 2 + ri) * (span - 1) + q // quarter]
                    here = q % quarter
                elif delta > cells:
                    source = messages[slots - delta - 1][ri * packs + h]
                    here = j
                else:
                    own = (c < half) == low
                    source = jnp.where(own, z_ref[main + ri], messages[cells - 1][ri])
                    here = c % half
                moved = pltpu.roll(source, (rows * (there - here + quarter)) % LANES, axis=1)
                old = acc_ref[group, c * 2 + ri]
                acc_ref[group, c * 2 + ri] = jnp.where(lane == there, moved, old)
        return carry

    lax.fori_loop(0, channels, body, 0)
    for g in range(slots // quarter):
        scale = scale_ref[:, g * LANES : (g + 1) * LANES]
        for c in range(channels):
            for ri in range(2):
                out_ref[:, c, ri, g * LANES : (g + 1) * LANES] = acc_ref[g, c * 2 + ri] * scale


def part_order(places):
    up = {}
    down = {}
    need = [dict() for _ in range(places)]
    for step in range(places - 1):
        for z in range(places):
            if z <= step:
                target = places - 1 - (step - z)
                up[step, z] = target
                need[z].setdefault(target, step)
            w = places - 1 - z
            if w <= step:
                target = step - w
                down[step, z] = target
                need[z].setdefault(target, step)
    order = [None] * places
    for z in range(places):
        slots = [None] * places
        slots[places - 1] = z
        for target, step in sorted(need[z].items(), key=lambda item: (item[1], -abs(item[0] - z))):
            free = [i for i in range(step, -1, -1) if slots[i] is None]
            slots[free[0]] = target
        order[z] = slots
    return order, up, down


def grid_shards(voltages, antenna_flags, owned_tile, places):
    slots = lax.axis_size("tm")
    me = lax.axis_index("tm")
    channels, _, inputs, samples = voltages.shape
    rows = inputs // slots
    subs = antenna_flags.shape[0]
    groups = inputs // LANES
    span = groups // 2 + 1
    half = channels // 2
    z, y, core = me // 4, (me // 2) % 2, me % 2
    order, up, down = part_order(places)
    order_table = jnp.array(order, jnp.int32)
    my_order = order_table[z]
    blocks = channels * 2 * (span - 1) + 2
    chunk = jax.ShapeDtypeStruct((2, blocks, rows, LANES), jnp.float32)
    chunk_spec = pl.BlockSpec((2, blocks, rows, LANES), lambda c: (0, 0, 0, 0))
    x_spec = pl.BlockSpec((1, 2, inputs, samples), lambda c: (c, 0, 0, 0))
    smem = pl.BlockSpec(memory_space=pltpu.SMEM)
    vmem = pl.BlockSpec(memory_space=pltpu.VMEM)
    size = dict(groups=groups, rows=rows, half=half)
    product = pltpu.VMEM((2 * LANES, span * LANES), jnp.float32)
    params = pltpu.CompilerParams(dimension_semantics=("arbitrary",))

    def place(i):
        return jnp.stack([my_order[i], y, core, me])

    masked, own, send = pl.pallas_call(
        lambda *refs: first_kernel(*refs, slots=slots, subs=subs, **size),
        grid=(channels,),
        in_specs=[smem, smem, smem, x_spec],
        out_specs=[x_spec, chunk_spec, chunk_spec],
        out_shape=[jax.ShapeDtypeStruct(voltages.shape, jnp.bfloat16), chunk, chunk],
        scratch_shapes=[pltpu.VMEM((inputs, samples), jnp.bfloat16), product],
        compiler_params=params,
        name="mask_and_part",
    )(place(0), owned_tile, antenna_flags, voltages)
    parts = [(own, send)]
    for i in range(1, places):
        parts.append(
            pl.pallas_call(
                lambda *refs: next_kernel(*refs, **size),
                grid=(channels,),
                in_specs=[smem, x_spec],
                out_specs=[chunk_spec, chunk_spec],
                out_shape=[chunk, chunk],
                scratch_shapes=[product],
                compiler_params=params,
                name="part",
            )(place(i), masked)
        )

    other_core = [(d, d ^ 1) for d in range(slots)]
    other_y = [(d, d ^ 2) for d in range(slots)]

    def along(pairs):
        return [(a * 4 + i, b * 4 + i) for a, b in pairs for i in range(4)]

    kept = []
    arrived = []
    for own, send in parts:
        got = lax.ppermute(send, "tm", other_core)
        kept.append(own[0] + got[0])
        arrived.append(lax.ppermute(own[1] + got[1], "tm", other_y))

    whole = [a + b for a, b in zip(kept[:-1], arrived[:-1])]

    def pick(step, table):
        wanted = {}
        for (s, place_z), target in table.items():
            if s == step:
                wanted.setdefault(order[place_z].index(target), []).append(place_z)
        choices = sorted(wanted.items(), key=lambda item: -len(item[1]))
        value = whole[choices[0][0]]
        for i, zs in choices[1:]:
            here = z == zs[0]
            for other in zs[1:]:
                here = here | (z == other)
            value = jnp.where(here, whole[i], value)
        return value

    from_below = None
    from_above = None
    for step in range(places - 1):
        going_up = pick(step, up)
        going_down = pick(step, down)
        if step:
            going_up = going_up + from_below
            going_down = going_down + from_above
        from_below = lax.ppermute(going_up, "tm", along([(s, s + 1) for s in range(step + 1)]))
        from_above = lax.ppermute(
            going_down, "tm", along([(places - 1 - s, places - 2 - s) for s in range(step + 1)])
        )

    cells = slots // 2
    packs = channels * rows // LANES
    message = [jax.ShapeDtypeStruct((2 * packs, rows, LANES), jnp.float32)] * (cells - 1)
    message.append(jax.ShapeDtypeStruct((2, rows, LANES), jnp.float32))
    reduced, *outgoing = pl.pallas_call(
        lambda *refs: mirror_kernel(*refs, channels=channels, rows=rows, slots=slots, span=span),
        in_specs=[smem] + [vmem] * 4,
        out_specs=[vmem] * (cells + 1),
        out_shape=[jax.ShapeDtypeStruct((blocks, rows, LANES), jnp.float32)] + message,
        scratch_shapes=[pltpu.VMEM((span - 1, 2 * packs, LANES, LANES), jnp.float32)],
        name="mirror",
    )(place(0), kept[-1], arrived[-1], from_below, from_above)
    incoming = [
        lax.ppermute(value, "tm", [(d, (d + delta) % slots) for d in range(slots)])
        for delta, value in enumerate(outgoing, 1)
    ]

    words = lax.all_gather(antenna_flags, "tm", axis=0, tiled=True)
    scale = pl.pallas_call(
        lambda *refs: scale_kernel(*refs, rows=rows, sub_length=samples // subs),
        in_specs=[smem, smem, vmem],
        out_specs=vmem,
        out_shape=jax.ShapeDtypeStruct((rows, inputs), jnp.float32),
        scratch_shapes=[pltpu.VMEM((inputs, inputs), jnp.float32)],
        name="scale",
    )(place(0), owned_tile, words)
    return pl.pallas_call(
        lambda *refs: final_kernel(*refs, channels=channels, rows=rows, slots=slots, span=span),
        in_specs=[smem, smem] + [vmem] * (2 + cells),
        out_specs=vmem,
        out_shape=jax.ShapeDtypeStruct((rows, channels, 2, inputs), jnp.float32),
        scratch_shapes=[pltpu.VMEM((groups, channels * 2, rows, LANES), jnp.float32)],
        name="assemble",
    )(place(0), owned_tile, reduced, scale, *incoming)


def solution(mesh):
    places = line_of_chips(mesh)

    def shards(voltages, antenna_flags, owned_tile):
        channels, _, inputs, samples = voltages.shape
        slots = mesh.shape["tm"]
        subs = antenna_flags.shape[0]
        rows = inputs // slots
        fits = (
            places is not None
            and rows * 4 == LANES
            and inputs == places * LANES
            and places % 2 == 0
            and channels % 4 == 0
            and channels * rows == 2 * LANES
            and samples == subs * LANES
        )
        if fits:
            return grid_shards(voltages, antenna_flags, owned_tile, places)
        return plain_shards(voltages, antenna_flags, owned_tile)

    return jax.shard_map(
        shards,
        mesh=mesh,
        in_specs=(P("band", None, None, "tm"), P("tm", "band"), P()),
        out_specs=P("tm", "band", None, None),
        check_vma=False,
    )
```

```python
import jax
import jax.numpy as jnp
from jax import lax
from jax.experimental import pallas as pl
from jax.experimental.pallas import tpu as pltpu
from jax.sharding import PartitionSpec as P


LANES = 128


def unpack_flags(words):
    shifts = jnp.arange(32, dtype=jnp.int32)
    bits = jnp.bitwise_and(jnp.right_shift(words[:, :, None], shifts[None, None, :]), 1)
    return bits.reshape(words.shape[0], words.shape[1] * 32)


def stack_operands(masked):
    real_part = masked[:, 0]
    imag_part = masked[:, 1]
    right_side = jnp.concatenate([real_part, imag_part], axis=-1)
    left_side = jnp.stack([right_side, jnp.concatenate([imag_part, -real_part], axis=-1)], axis=1)
    return (left_side, right_side)


def plain_shards(voltages, antenna_flags, owned_tile):
    axis_count = lax.axis_size("tm")
    my_index = lax.axis_index("tm")
    inputs = voltages.shape[2]
    samples = voltages.shape[3]
    block_rows = inputs // axis_count
    sub_length = samples // antenna_flags.shape[0]
    every_word = lax.all_gather(antenna_flags, "tm", axis=0, tiled=True)
    every_flag = unpack_flags(every_word)
    local_flag = unpack_flags(antenna_flags)
    own_tile = owned_tile[my_index]
    own_antennas = (own_tile * block_rows + jnp.arange(block_rows, dtype=jnp.int32)) // 2
    own_flags = jnp.take(every_flag, own_antennas, axis=1)
    input_flags = jnp.repeat(every_flag, 2, axis=1)
    counts = sub_length * jnp.dot(own_flags.T, input_flags)
    divisor = jnp.maximum(counts, 1).astype(jnp.float32)[:, None, None, :]
    sample_flags = jnp.repeat(jnp.repeat(local_flag, 2, axis=1).T, sub_length, axis=1).astype(
        jnp.bfloat16
    )
    masked = voltages * sample_flags[None, None]
    left_side, right_side = stack_operands(masked)
    row_index = (
        owned_tile[:, None] * block_rows + jnp.arange(block_rows, dtype=jnp.int32)[None, :]
    ).reshape(-1)
    picked = jnp.take(left_side, row_index, axis=2)
    summed = lax.psum_scatter(
        jnp.einsum("ckru,cju->rckj", picked, right_side, preferred_element_type=jnp.float32),
        "tm",
        scatter_dimension=0,
        tiled=True,
    )
    return summed / divisor


def line_of_chips(mesh):
    columns = mesh.devices.reshape(-1, mesh.shape["tm"])
    count = columns.shape[1]
    if count % 4:
        return None
    for column in columns:
        places = []
        for device in column:
            coords = getattr(device, "coords", None)
            core = getattr(device, "core_on_chip", None)
            if coords is None or core is None:
                return None
            places.append((coords[2], coords[1], coords[0], core))
        zs = sorted({p[0] for p in places})
        ys = sorted({p[1] for p in places})
        if len(ys) != 2 or len({p[2] for p in places}) != 1 or len(zs) * 4 != count:
            return None
        want = [(z, y, places[0][2], core) for z in zs for y in ys for core in (0, 1)]
        if places != want:
            return None
    return count // 4


def fill_mask(mask_ref, tile_ref, flag_ref, slots, rows, subs, sub_length):
    antennas = rows // 2
    row = lax.broadcasted_iota(jnp.int32, (rows, sub_length), 0)
    for k in range(slots):
        first = tile_ref[k] * antennas
        shift = first % 32 + row // 2
        for s in range(subs):
            word = flag_ref[s, first // 32]
            bit = lax.shift_right_arithmetic(jnp.full((rows, sub_length), word, jnp.int32), shift) & 1
            mask_ref[k * rows : (k + 1) * rows, s * sub_length : (s + 1) * sub_length] = bit.astype(
                jnp.float32
            ).astype(jnp.bfloat16)


def gram_step(c, x_ref, T, y, core, store, load, p_ref, *, groups, rows, channels):
    quarter = LANES // rows
    span = groups // 2 + 1

    def both(g):
        at = pl.ds(pl.multiple_of(g * LANES, LANES), LANES)
        return x_ref[c, 0, at, :], x_ref[c, 1, at, :]

    real, imag = both(T)
    left = jnp.concatenate(
        [jnp.concatenate([real, imag], axis=1), jnp.concatenate([imag, -real], axis=1)], axis=0
    )
    right = jnp.concatenate(
        [jnp.concatenate(both((T + g) % groups), axis=1) for g in range(span)], axis=0
    )
    p_ref[...] = lax.dot_general(
        left, right, (((1,), (1,)), ((), ())), preferred_element_type=jnp.float32
    )
    lane = lax.broadcasted_iota(jnp.int32, (rows, LANES), 1)
    edge = slice((span - 1) * LANES, span * LANES)
    j = c % quarter
    tail = channels * 2 * (span - 1) + c // quarter
    for dest, parity in ((0, core), (1, 1 - core)):
        for slot_y in range(2):
            r = 2 * (y if slot_y == 0 else 1 - y) + parity
            shift = r * rows
            for ri in range(2):
                at = pl.ds(pl.multiple_of(ri * LANES + shift, rows), rows)
                last = p_ref[at, edge]
                for g in range(span - 1):
                    block = p_ref[at, g * LANES : (g + 1) * LANES]
                    if g == 0:
                        block = jnp.where(lane < shift, last, block)
                    store(dest, slot_y, (c * 2 + ri) * (span - 1) + g, block)
            across = jnp.where(T < groups // 2, 0, LANES)
            last = p_ref[pl.ds(pl.multiple_of(across + shift, rows), rows), edge]
            moved = pltpu.roll(last, (rows * (j - r + quarter)) % LANES, axis=1)
            old = load(dest, slot_y, tail)
            store(dest, slot_y, tail, jnp.where(lane // rows == j, moved, old))


def my_place(places):
    me = lax.axis_index("tm")
    z = me // 4
    order = []
    for i in range(places):
        target = jnp.int32(ORDER[0][i])
        for other in range(1, places):
            target = jnp.where(z == other, ORDER[other][i], target)
        order.append(target)
    return order + [(me // 2) % 2, me % 2, me]


def first_kernel(
    tile_ref, flag_ref, v_ref, x_ref, own_ref, send_ref, word_ref, raw_ref, mask_ref, p_ref, sems, *, slots, subs, **kw
):
    channels, rows = kw["channels"], kw["rows"]

    def fetch(c):
        return pltpu.make_async_copy(v_ref.at[c], raw_ref.at[c], sems.at[c])

    for c in range(channels):
        fetch(c).start()
    fill_mask(mask_ref, tile_ref, flag_ref, slots, rows, subs, v_ref.shape[3] // subs)
    spread = word_ref.shape
    here = lax.broadcasted_iota(jnp.int32, spread, 0) - lax.axis_index("tm") * subs
    column = lax.broadcasted_iota(jnp.int32, spread, 1)
    words = jnp.zeros(spread, jnp.int32)
    for sub in range(subs):
        for w in range(spread[1]):
            words = jnp.where((here == sub) & (column == w), flag_ref[sub, w], words)
    word_ref[...] = words
    places = len(ORDER)
    place_ref = my_place(places)
    refs = (own_ref, send_ref)

    def store(dest, slot_y, block, value):
        refs[dest][slot_y, block] = value

    def load(dest, slot_y, block):
        return refs[dest][slot_y, block]

    def body(c, carry):
        fetch(c).wait()
        for k in range(slots):
            at = pl.ds(pl.multiple_of(tile_ref[k] * rows, rows), rows)
            for ri in range(2):
                x_ref[c, ri, k * rows : (k + 1) * rows, :] = (
                    raw_ref[c, ri, at, :] * mask_ref[k * rows : (k + 1) * rows, :]
                )
        gram_step(c, x_ref, place_ref[0], place_ref[places], place_ref[places + 1], store, load, p_ref, **kw)
        return carry

    lax.fori_loop(0, channels, body, 0)


def next_kernel(x_ref, own_ref, send_ref, p_ref, *, part, **kw):
    places = len(ORDER)
    place_ref = my_place(places)
    refs = (own_ref, send_ref)

    def store(dest, slot_y, block, value):
        refs[dest][slot_y, block] = value

    def load(dest, slot_y, block):
        return refs[dest][slot_y, block]

    def body(c, carry):
        gram_step(c, x_ref, place_ref[part], place_ref[places], place_ref[places + 1], store, load, p_ref, **kw)
        return carry

    lax.fori_loop(0, kw["channels"], body, 0)


def join_kernel(own_ref, got_ref, away_ref, kept_ref):
    away_ref[...] = own_ref[1] + got_ref[1]
    kept_ref[...] = own_ref[0] + got_ref[0]


def sum_kernel(*refs):
    total = refs[0][...] + refs[1][...]
    for ref in refs[2:-1]:
        total = total + ref[...]
    refs[-1][...] = total


def mirror_kernel(a_ref, b_ref, c_ref, d_ref, e_ref, z_ref, *refs, channels, rows, slots, span):
    messages, tr_ref = refs[:-1], refs[-1]
    places = len(ORDER)
    place_ref = my_place(places)
    r = place_ref[places] * 2 + place_ref[places + 1]
    quarter = LANES // rows
    cells = (span - 1) * quarter
    z_ref[...] = (a_ref[...] + b_ref[...]) + ((c_ref[...] + d_ref[...]) + e_ref[...])
    packs = channels // quarter
    for ri in range(2):
        for g in range(span - 1):
            for h in range(packs):
                block = jnp.concatenate(
                    [z_ref[((h * quarter + j) * 2 + ri) * (span - 1) + g] for j in range(quarter)], axis=0
                )
                turned = block.T
                tr_ref[g, ri * packs + h] = -turned if ri else turned
    for delta in range(1, cells):
        q = (r + delta) % cells
        at = pl.ds(pl.multiple_of((q % quarter) * rows, rows), rows)
        for i in range(2 * packs):
            messages[delta - 1][i] = tr_ref[q // quarter, i, at, :]
    lane = lax.broadcasted_iota(jnp.int32, (rows, LANES), 1)
    main = channels * 2 * (span - 1)
    low = place_ref[places + 2] < slots // 2
    for h in range(packs):
        turned = jnp.concatenate([z_ref[main + h]] * quarter, axis=0).T
        piece = turned[0:rows]
        for j in range(1, quarter):
            piece = jnp.where(lane // rows == j, turned[j * rows : (j + 1) * rows], piece)
        messages[cells - 1][h] = jnp.where(low, piece, -piece)


def scale_kernel(tile_ref, word_ref, out_ref, count_ref, *, rows, sub_length):
    inputs = out_ref.shape[1]
    words = word_ref[...]
    subs = words.shape[0]
    lane = lax.broadcasted_iota(jnp.int32, (subs, LANES), 1)
    parts = []
    for g in range(inputs // LANES):
        low, high = words[:, 2 * g : 2 * g + 1], words[:, 2 * g + 1 : 2 * g + 2]
        word = jnp.where(lane < LANES // 2, low, high)
        parts.append(lax.shift_right_arithmetic(word, (lane % (LANES // 2)) // 2) & 1)
    good = jnp.concatenate(parts, axis=1).astype(jnp.float32).astype(jnp.bfloat16)
    count_ref[...] = lax.dot_general(
        good, good, (((0,), (0,)), ((), ())), preferred_element_type=jnp.float32
    )
    me = lax.axis_index("tm")
    first = pl.multiple_of(tile_ref[me] * rows, rows)
    counts = count_ref[pl.ds(first, rows), :] * float(sub_length)
    out_ref[...] = 1.0 / jnp.maximum(counts, 1.0)


def final_kernel(tile_ref, z_ref, scale_ref, *refs, channels, rows, slots, span):
    quarter = LANES // rows
    cells = (span - 1) * quarter
    packs = channels // quarter
    main = channels * 2 * (span - 1)
    messages, out_ref, all_ref, slot_ref = refs[:cells], refs[cells], refs[cells + 1], refs[cells + 2]
    places = len(ORDER)
    place_ref = my_place(places)
    me = place_ref[places + 2]
    r = place_ref[places] * 2 + place_ref[places + 1]
    lane = lax.broadcasted_iota(jnp.int32, (rows, LANES), 1) // rows
    low = jnp.where(me < slots // 2, 1, 0)
    first = main + packs
    all_ref[0:first] = z_ref[...]
    for delta in range(1, cells):
        at = first + (delta - 1) * 2 * packs
        all_ref[at : at + 2 * packs] = messages[delta - 1][...]
    last = first + (cells - 1) * 2 * packs
    all_ref[last : last + packs] = messages[cells - 1][...]
    for k in range(slots):
        slot_ref[tile_ref[k]] = k

    def body(c, carry):
        j = c % quarter
        h = c // quarter
        for group in range(slots // quarter):
            pieces = [[], []]
            for there in range(quarter):
                delta = (slot_ref[group * quarter + there] - me + slots) % slots
                q = (r + delta) % cells
                ahead = delta < cells
                behind = delta > cells
                here = jnp.where(ahead, q % quarter, j)
                shift = (rows * (there - here + quarter)) % LANES
                for ri in range(2):
                    mine = low if ri == 0 else 1 - low
                    at = jnp.where(
                        ahead,
                        (c * 2 + ri) * (span - 1) + q // quarter,
                        jnp.where(
                            behind,
                            first + (slots - 1 - delta) * 2 * packs + ri * packs + h,
                            jnp.where(mine == 1, main, last) + h,
                        ),
                    )
                    pieces[ri].append(pltpu.roll(all_ref[at], shift, axis=1))
            scale = scale_ref[:, group * LANES : (group + 1) * LANES]
            for ri in range(2):
                value = pieces[ri][0]
                for there in range(1, quarter):
                    value = jnp.where(lane == there, pieces[ri][there], value)
                out_ref[:, c, ri, group * LANES : (group + 1) * LANES] = value * scale
        return carry

    for c in range(channels):
        body(c, 0)


ORDER = ((3, 2, 1, 0), (0, 3, 2, 1), (3, 0, 1, 2), (0, 1, 2, 3))
HOPS = (2, 1, 4, 8)


def inverse_counts(words, owned_tile, slots, rows, inputs, sub_length):
    smem = pl.BlockSpec(memory_space=pltpu.SMEM)
    vmem = pl.BlockSpec(memory_space=pltpu.VMEM)
    for hop in HOPS:
        words = words + lax.ppermute(words, "tm", [(d, d ^ hop) for d in range(slots)])
    return pl.pallas_call(
        lambda *refs: scale_kernel(*refs, rows=rows, sub_length=sub_length),
        in_specs=[smem, vmem],
        out_specs=vmem,
        out_shape=jax.ShapeDtypeStruct((rows, inputs), jnp.float32),
        scratch_shapes=[pltpu.VMEM((inputs, inputs), jnp.float32)],
        compiler_params=pltpu.CompilerParams(vmem_limit_bytes=4 << 20),
        name="scale",
    )(owned_tile, words)


def grid_shards(voltages, antenna_flags, owned_tile, places):
    slots = lax.axis_size("tm")
    channels, _, inputs, samples = voltages.shape
    rows = inputs // slots
    subs = antenna_flags.shape[0]
    groups = inputs // LANES
    span = groups // 2 + 1
    quarter = LANES // rows
    packs = channels // quarter
    blocks = channels * 2 * (span - 1) + packs
    smem = pl.BlockSpec(memory_space=pltpu.SMEM)
    vmem = pl.BlockSpec(memory_space=pltpu.VMEM)
    size = dict(groups=groups, rows=rows, channels=channels)
    product = pltpu.VMEM((2 * LANES, span * LANES), jnp.float32)

    work = 4 * channels * LANES * inputs * samples * 8

    def chunk(*lead):
        return jax.ShapeDtypeStruct(lead + (blocks, rows, LANES), jnp.float32)

    def limit(mib):
        return pltpu.CompilerParams(vmem_limit_bytes=mib << 20)

    masked, own, send, words = pl.pallas_call(
        lambda *refs: first_kernel(*refs, slots=slots, subs=subs, **size),
        in_specs=[smem, smem, pl.BlockSpec(memory_space=pltpu.HBM)],
        out_specs=[vmem] * 4,
        out_shape=[jax.ShapeDtypeStruct(voltages.shape, jnp.bfloat16), chunk(2), chunk(2), jax.ShapeDtypeStruct((slots * subs, antenna_flags.shape[1]), jnp.int32)],
        scratch_shapes=[
            pltpu.VMEM(voltages.shape, jnp.bfloat16),
            pltpu.VMEM((inputs, samples), jnp.bfloat16),
            product,
            pltpu.SemaphoreType.DMA((channels,)),
        ],
        compiler_params=limit(16),
        cost_estimate=pl.CostEstimate(flops=work, bytes_accessed=0, transcendentals=0),
        name="mask_and_part",
    )(owned_tile, antenna_flags, pltpu.with_memory_space_constraint(voltages, pltpu.HBM))
    parts = [(own, send)]
    for i in range(1, places):
        parts.append(
            pl.pallas_call(
                lambda *refs: next_kernel(*refs, part=i, **size),
                in_specs=[vmem],
                out_specs=[vmem] * 2,
                out_shape=[chunk(2)] * 2,
                scratch_shapes=[product],
                compiler_params=limit(16),
                cost_estimate=pl.CostEstimate(flops=work, bytes_accessed=0, transcendentals=0),
            )(masked)
        )

    other_core = [(d, d ^ 1) for d in range(slots)]
    other_y = [(d, d ^ 2) for d in range(slots)]

    def along(pairs):
        return [(a * 4 + i, b * 4 + i) for a, b in pairs for i in range(4)]

    def send_to(value, pairs):
        return lax.ppermute(value, "tm", pairs)

    arrived, kept = [], []
    for i, (own, send) in enumerate(parts):
        got = send_to(send, other_core)
        away, stays = pl.pallas_call(
            join_kernel, in_specs=[vmem] * 2, out_specs=[vmem] * 2, out_shape=[chunk()] * 2, compiler_params=limit(8)
        )(own, got)
        kept.append(stays)
        arrived.append(send_to(away, other_y))

    def added(*values):
        return pl.pallas_call(
            sum_kernel, in_specs=[vmem] * len(values), out_specs=vmem, out_shape=chunk(), compiler_params=limit(8)
        )(*values)

    scale = inverse_counts(words, owned_tile, slots, rows, inputs, samples // subs)
    inwards = along([(0, 1), (3, 2)])
    across = along([(1, 2), (2, 1)])
    outwards = along([(1, 0), (2, 3)])
    first = added(kept[0], arrived[0])
    end0 = send_to(first, inwards)
    second = added(kept[1], arrived[1])
    end1 = send_to(second, inwards)
    mid1 = send_to(added(second, end0), across)
    third = added(kept[2], arrived[2])
    end2 = send_to(third, inwards)
    mid2 = send_to(added(third, end1), across)
    back = send_to(added(first, mid1), outwards)

    cells = slots // 2
    message = [jax.ShapeDtypeStruct((2 * packs, rows, LANES), jnp.float32)] * (cells - 1)
    message.append(jax.ShapeDtypeStruct((packs, rows, LANES), jnp.float32))
    reduced, *outgoing = pl.pallas_call(
        lambda *refs: mirror_kernel(*refs, channels=channels, rows=rows, slots=slots, span=span),
        in_specs=[vmem] * 5,
        out_specs=[vmem] * (cells + 1),
        out_shape=[chunk()] + message,
        scratch_shapes=[pltpu.VMEM((span - 1, 2 * packs, LANES, LANES), jnp.float32)],
        compiler_params=limit(8),
        name="mirror",
    )(kept[-1], arrived[-1], end2, mid2, back)
    incoming = [
        send_to(value, [(d, (d + delta) % slots) for d in range(slots)])
        for delta, value in enumerate(outgoing, 1)
    ]
    return pl.pallas_call(
        lambda *refs: final_kernel(*refs, channels=channels, rows=rows, slots=slots, span=span),
        in_specs=[smem] + [vmem] * (2 + cells),
        out_specs=vmem,
        out_shape=jax.ShapeDtypeStruct((rows, channels, 2, inputs), jnp.float32),
        scratch_shapes=[
            pltpu.VMEM((blocks + 2 * packs * (cells - 1) + packs, rows, LANES), jnp.float32),
            pltpu.SMEM((slots,), jnp.int32),
        ],
        compiler_params=limit(12),
        name="assemble",
    )(owned_tile, reduced, scale, *incoming)


def solution(mesh):
    places = line_of_chips(mesh)

    def shards(voltages, antenna_flags, owned_tile):
        channels, _, inputs, samples = voltages.shape
        slots = mesh.shape["tm"]
        subs = antenna_flags.shape[0]
        rows = inputs // slots
        fits = (
            places is not None
            and rows * 4 == LANES
            and inputs == places * LANES
            and places == len(ORDER)
            and channels % (LANES // rows) == 0
            and slots & (slots - 1) == 0
            and samples == subs * LANES
        )
        if fits:
            return grid_shards(voltages, antenna_flags, owned_tile, places)
        return plain_shards(voltages, antenna_flags, owned_tile)

    return jax.shard_map(
        shards,
        mesh=mesh,
        in_specs=(P("band", None, None, "tm"), P("tm", "band"), P()),
        out_specs=P("tm", "band", None, None),
        check_vma=False,
    )
```
